32 devices in a mesh: snap: 4 (over z), param: 8 (over y, x, core).
Axes of the slice: x: 2, y: 2, z: 4, core: 2. Of those that a mesh axis runs over, the one named last changes fastest.
Arguments:
- snapshots: bfloat16 [256, 512, 1024], P('snap', 'param'), as said below
- coeffs: float32 [16, 256], P(None, 'snap'), may hold values from -0.375 to 0.375
Outputs:
- averages: float32 [16, 512, 1024], P(None, 'param', 'snap')
- width_norms: float32 [16], replicated
The draws below stay inside these ranges and needn't reach their ends.
Inputs may be any that keep to these rules, and one draw needn't show every extreme that they name: `snapshots`: stored snapshot weights, finite.
All inputs are finite; a program needn't handle non-finite values.
Results may differ from the reference program's by a relative error of at most 0.0003.
Values may be sent and summed in bfloat16 or wider, within the bound.
A program may use at most 64 MiB of HBM per device.

```python
import math
import jax
import jax.numpy as jnp
from jax import lax

WIDTHS = 16
COLS = 1024
NSNAP = 256
ROWS = 512


def draw_snapshots(key, part):
    key_rows = jax.random.fold_in(key, 11)
    key_cols = jax.random.fold_in(key, 12)
    key_base = jax.random.fold_in(key, 13)
    row_index = jnp.arange(ROWS, dtype=jnp.float32)
    row_scale = 3.0 ** (row_index / ROWS) * 10.0 ** jax.random.uniform(key_rows, (ROWS,), jnp.float32)
    col_scale = 10.0 ** jax.random.uniform(key_cols, (COLS,), jnp.float32)
    base = jax.random.normal(key_base, (NSNAP, ROWS, COLS), jnp.float32)
    values = base * row_scale[None, :, None] * col_scale[None, None, :] / 10.0
    return values.astype(jnp.bfloat16)


def block_scale(key, shape, shards, least, largest):
    loudness, own = 1.0, jax.random.fold_in(key, 6)
    for dim, blocks in shards:
        draws = jnp.exp(jax.random.uniform(jax.random.fold_in(own, dim), (blocks,), jnp.float32, least / len(shards), largest / len(shards)))
        loudness = loudness * jnp.repeat(draws, shape[dim] // blocks).reshape([-1 if axis == dim else 1 for axis in range(len(shape))])
    return loudness


def gaussian(rng, extent, deviation, most, cuts=(), kind=jnp.bfloat16):
    values = jax.random.normal(rng, extent, jnp.float32) * deviation
    if len(cuts) > 0:
        values = block_scale(rng, extent, cuts, -0.22, 0.18) * values
    return jnp.clip(values, min=-most, max=most).astype(kind)


def setup_inputs(seed: int = 0) -> dict:
    splits = jax.random.split(jax.random.key(seed), 3)
    snapshots = draw_snapshots(jax.random.fold_in(splits[2], 71), 0)
    coeffs = gaussian(splits[1], (WIDTHS, NSNAP), NSNAP ** -0.5, 0.375, ((1, 4),), jnp.float32)
    return dict(snapshots=snapshots, coeffs=coeffs)


def reference(snapshots, coeffs):
    block_rows = math.gcd(ROWS, 256)
    block_count = ROWS // block_rows

    def one_block(block_index):
        start = (block_index * block_rows).astype(jnp.int32)
        piece = lax.dynamic_slice_in_dim(snapshots, start, block_rows, 1).astype(jnp.float32)
        flat = piece.reshape(NSNAP, block_rows * COLS)
        product = jnp.dot(coeffs.astype(jnp.float32), flat, precision=lax.Precision.HIGHEST, preferred_element_type=jnp.float32)
        return product.reshape(WIDTHS, block_rows, COLS)
    stacked = lax.map(one_block, jnp.arange(block_count, dtype=jnp.int32))
    averages = jnp.transpose(stacked, (1, 0, 2, 3)).reshape(WIDTHS, ROWS, COLS)
    squares = lax.optimization_barrier(jnp.sum(averages * averages, axis=(1, 2)))
    width_norms = jnp.sqrt(squares / jnp.float32(ROWS * COLS))
    return (averages, width_norms)
```

```python
import functools

import jax
import jax.numpy as jnp
from jax import lax
from jax.experimental import pallas as pl
from jax.experimental.pallas import tpu as pltpu
from jax.sharding import PartitionSpec as P

MESH = pl.DeviceIdType.MESH
GROUP = 16
LAG = 2
POWER = 15
TOP = 2.0**8.375


def encode(value):
    largest = jnp.max(jnp.max(jnp.abs(value), axis=0), axis=0, keepdims=True)
    largest = jnp.maximum(largest, 1e-30)
    x = value * (TOP / largest)[None]
    x2 = x * x
    x4 = x2 * x2
    x8 = x4 * x4
    return ((x8 * x4) * (x2 * x)).astype(jnp.bfloat16), largest * (1.0 / TOP)


def decode(code, scale):
    y = code.astype(jnp.float32)
    size = jnp.exp2(jnp.log2(jnp.maximum(jnp.abs(y), 1e-38)) * (1.0 / POWER)) * scale[None]
    return jnp.where(y > 0.0, size, jnp.where(y < 0.0, -size, 0.0))


def kernel(
    n, peers, entries, coeffs, stored, averages, norms,
    spread, tiles, part, out_code, out_scale, in_code, in_scale, rows, planes,
    load_sem, send_sem, send_scale_sem, recv_sem, recv_scale_sem,
    row_send, row_recv, plane_send, plane_recv,
):
    z = lax.axis_index("snap")
    me = lax.axis_index("param")
    widths, count = coeffs.shape
    keep = stored.shape[2] // n
    groups = stored.shape[1] // GROUP
    steps = (n - 1) * groups
    low = z < n // 2

    barrier = pltpu.get_barrier_semaphore()
    for k in range(1, n):
        pl.semaphore_signal(barrier, inc=1, device_id={"snap": lax.rem(z + k, n)}, device_id_type=MESH)

    @pl.loop(1, peers)
    def _(k):
        pl.semaphore_signal(barrier, inc=1, device_id={"param": lax.rem(me + k, peers)}, device_id_type=MESH)

    def load(i):
        q, t = i // groups, lax.rem(i, groups)
        d = jnp.where(low, n - 1 - q, q)
        return pltpu.make_async_copy(
            stored.at[:, pl.ds(pl.multiple_of(t * GROUP, GROUP), GROUP), pl.ds(pl.multiple_of(d * keep, keep), keep)],
            tiles.at[i],
            load_sem.at[i],
        )

    @pl.loop(0, n * groups)
    def _(i):
        load(i).start()

    exact = coeffs[...]
    high = exact.astype(jnp.bfloat16)
    rest = (exact - high.astype(jnp.float32)).astype(jnp.bfloat16)
    both = jnp.concatenate([high, rest], axis=0)
    tall, wide = spread.shape
    row = lax.broadcasted_iota(jnp.int32, (tall, 2 * widths), 0)
    col = lax.broadcasted_iota(jnp.int32, (tall, 2 * widths), 1)
    pick = jnp.where(row // GROUP == col, 1.0, 0.0).astype(jnp.bfloat16)
    row = lax.broadcasted_iota(jnp.int32, (count, wide), 0)
    col = lax.broadcasted_iota(jnp.int32, (count, wide), 1)
    repeat = jnp.where(col // GROUP == row, 1.0, 0.0).astype(jnp.bfloat16)
    tall_rows = jnp.dot(pick, both, preferred_element_type=jnp.float32).astype(jnp.bfloat16)
    full = jnp.dot(tall_rows, repeat, preferred_element_type=jnp.float32)
    row = lax.broadcasted_iota(jnp.int32, (tall, wide), 0)
    col = lax.broadcasted_iota(jnp.int32, (tall, wide), 1)
    spread[...] = jnp.where(row % GROUP == col % GROUP, full, 0.0).astype(jnp.bfloat16)

    pl.semaphore_wait(barrier, n - 1 + peers - 1)

    def copies(way, k, peer):
        code = pltpu.make_async_remote_copy(
            src_ref=out_code.at[way, k], dst_ref=in_code.at[way, k],
            send_sem=send_sem.at[way, k], recv_sem=recv_sem.at[way, k],
            device_id={"snap": peer}, device_id_type=MESH,
        )
        scale = pltpu.make_async_remote_copy(
            src_ref=out_scale.at[way, k], dst_ref=in_scale.at[way, k],
            send_sem=send_scale_sem.at[way, k], recv_sem=recv_scale_sem.at[way, k],
            device_id={"snap": peer}, device_id_type=MESH,
        )
        return scale, code

    def send(way, k, peer, value):
        code, scale = encode(value)
        out_code[way, k] = code
        out_scale[way, k] = scale
        for copy in copies(way, k, peer):
            copy.start()

    half = widths * GROUP

    @pl.loop(0, n * groups)
    def _(i):
        q, t = i // groups, lax.rem(i, groups)
        d = jnp.where(low, n - 1 - q, q)
        load(i).wait()
        both_parts = jnp.dot(
            spread[...], tiles[i].reshape(count * GROUP, keep), preferred_element_type=jnp.float32
        )
        value = (both_parts[:half] + both_parts[half:]).reshape(widths, GROUP, keep)
        part[d, t] = value

        @pl.when(jnp.logical_and(jnp.logical_or(z == 0, z == n - 1), d != z))
        def _():
            way = jnp.where(z == 0, 0, 1)
            peer = jnp.where(z == 0, 1, n - 2)
            send(way, i, peer, value)

    def pass_on(way, k, d, peer):
        t = lax.rem(k, groups)
        for copy in copies(way, k, peer):
            copy.wait_recv()
        value = part[d, t] + decode(in_code[way, k], in_scale[way, k])

        @pl.when(d == z)
        def _():
            part[d, t] = value

        @pl.when(d != z)
        def _():
            send(way, k, peer, value)

    @pl.loop(0, steps)
    def _(j):
        up = j - LAG * (z - 1)

        @pl.when(jnp.logical_and(z > 0, jnp.logical_and(up >= 0, up < (n - z) * groups)))
        def _():
            pass_on(0, up, n - 1 - up // groups, jnp.where(z == n - 1, z - 1, z + 1))

        down = j - LAG * (n - 2 - z)

        @pl.when(jnp.logical_and(z < n - 1, jnp.logical_and(down >= 0, down < (z + 1) * groups)))
        def _():
            pass_on(1, down, down // groups, jnp.where(z == 0, z + 1, z - 1))

    sums = jnp.zeros((widths, 1), jnp.float32)
    for t in range(groups):
        value = part[z, t]
        averages[:, t * GROUP : (t + 1) * GROUP, :] = value
        sums += jnp.sum(jnp.sum(value * value, axis=1), axis=1, keepdims=True)
    lanes = norms.shape[1]
    row = lax.broadcasted_iota(jnp.int32, (widths, lanes), 0)
    col = lax.broadcasted_iota(jnp.int32, (widths, lanes), 1)
    line = jnp.sum(jnp.where(row == col, sums, 0.0), axis=0, keepdims=True)

    def share(buffer, sends, recvs, axis, mine, size, value):
        buffer[mine] = value

        def copy(k, slot):
            return pltpu.make_async_remote_copy(
                src_ref=buffer.at[slot], dst_ref=buffer.at[slot],
                send_sem=sends.at[k], recv_sem=recvs.at[slot],
                device_id={axis: lax.rem(mine + k, size)}, device_id_type=MESH,
            )

        @pl.loop(1, size)
        def _(k):
            copy(k, mine).start()

        @pl.loop(1, size)
        def _(k):
            copy(k, lax.rem(mine + k, size)).wait_recv()

        @pl.loop(1, size)
        def _(k):
            copy(k, mine).wait_send()

        return jnp.sum(buffer[...], axis=0)

    line = share(rows, row_send, row_recv, "param", me, peers, line)
    line = share(planes, plane_send, plane_recv, "snap", z, n, line)
    norms[...] = jnp.sqrt(line / jnp.float32(entries))

    @pl.loop(0, steps)
    def _(k):
        @pl.when(k < (n - 1 - z) * groups)
        def _():
            for copy in copies(0, k, jnp.where(z == n - 1, z - 1, z + 1)):
                copy.wait_send()

        @pl.when(k < z * groups)
        def _():
            for copy in copies(1, k, jnp.where(z == 0, z + 1, z - 1)):
                copy.wait_send()


def on_device(n, peers, snapshots, coeffs):
    count, height, cols = snapshots.shape
    widths = coeffs.shape[0]
    keep = cols // n
    groups = height // GROUP
    steps = (n - 1) * groups
    entries = height * cols * peers
    dma = pltpu.SemaphoreType.DMA
    averages, norms = pl.pallas_call(
        functools.partial(kernel, n, peers, entries),
        out_shape=(
            jax.ShapeDtypeStruct((widths, height, keep), jnp.float32),
            jax.ShapeDtypeStruct((1, 128), jnp.float32),
        ),
        in_specs=[pl.BlockSpec(memory_space=pltpu.VMEM), pl.BlockSpec(memory_space=pl.ANY)],
        out_specs=(pl.BlockSpec(memory_space=pltpu.VMEM), pl.BlockSpec(memory_space=pltpu.VMEM)),
        scratch_shapes=[
            pltpu.VMEM((2 * widths * GROUP, count * GROUP), jnp.bfloat16),
            pltpu.VMEM((n * groups, count, GROUP, keep), jnp.bfloat16),
            pltpu.VMEM((n, groups, widths, GROUP, keep), jnp.float32),
            pltpu.VMEM((2, steps, widths, GROUP, keep), jnp.bfloat16),
            pltpu.VMEM((2, steps, 1, keep), jnp.float32),
            pltpu.VMEM((2, steps, widths, GROUP, keep), jnp.bfloat16),
            pltpu.VMEM((2, steps, 1, keep), jnp.float32),
            pltpu.VMEM((peers, 1, 128), jnp.float32),
            pltpu.VMEM((n, 1, 128), jnp.float32),
            dma((n * groups,)),
            dma((2, steps)), dma((2, steps)), dma((2, steps)), dma((2, steps)),
            dma((peers,)), dma((peers,)), dma((n,)), dma((n,)),
        ],
        compiler_params=pltpu.CompilerParams(
            collective_id=0, has_side_effects=True, vmem_limit_bytes=48 * 1024 * 1024
        ),
        name="reconstruct",
    )(coeffs, snapshots)
    return averages, norms[0, :widths]


def solution(mesh):
    in_specs = (P("snap", "param", None), P(None, "snap"))
    out_specs = (P(None, "param", "snap"), P())
    body = functools.partial(on_device, mesh.shape["snap"], mesh.shape["param"])
    return jax.shard_map(body, mesh=mesh, in_specs=in_specs, out_specs=out_specs, check_vma=False)
```

```python
import functools

import jax
import jax.numpy as jnp
from jax import lax
from jax.experimental import pallas as pl
from jax.experimental.pallas import tpu as pltpu
from jax.sharding import PartitionSpec as P

MESH = pl.DeviceIdType.MESH
GROUP = 16
LAG = 3
POWER = 15
AHEAD = 4
TOP = 2.0**8.375


def encode(value):
    largest = jnp.max(jnp.max(jnp.abs(value), axis=0), axis=0, keepdims=True)
    largest = jnp.maximum(largest, 1e-30)
    x = value * (TOP / largest)[None]
    x2 = x * x
    x4 = x2 * x2
    x8 = x4 * x4
    return ((x8 * x4) * (x2 * x)).astype(jnp.bfloat16), largest * (1.0 / TOP)


def decode(code, scale):
    y = code.astype(jnp.float32)
    size = jnp.exp2(jnp.log2(jnp.maximum(jnp.abs(y), 1e-38)) * (1.0 / POWER)) * scale[None]
    return jnp.where(y > 0.0, size, jnp.where(y < 0.0, -size, 0.0))


def kernel(
    n, peers, entries, coeffs, stored, averages, norms,
    exact, spread, tiles, part, out_code, out_scale, in_code, in_scale, squares, lines,
    exact_sem, load_sem, send_sem, send_scale_sem, recv_sem, recv_scale_sem,
    line_send, line_recv, known,
):
    z = lax.axis_index("snap")
    me = lax.axis_index("param")
    widths, count = coeffs.shape
    keep = stored.shape[2] // n
    groups = stored.shape[1] // GROUP
    steps = (n - 1) * groups
    lag = min(LAG, groups - 1)
    low = z < n // 2

    barrier = pltpu.get_barrier_semaphore()
    for k in range(1, n):
        pl.semaphore_signal(barrier, inc=1, device_id={"snap": lax.rem(z + k, n)}, device_id_type=MESH)

    @pl.loop(1, peers)
    def _(k):
        pl.semaphore_signal(barrier, inc=1, device_id={"param": lax.rem(me + k, peers)}, device_id_type=MESH)

    def load(i):
        q, t = i // groups, lax.rem(i, groups)
        d = jnp.where(low, n - 1 - q, q)
        return pltpu.make_async_copy(
            stored.at[:, pl.ds(pl.multiple_of(t * GROUP, GROUP), GROUP), pl.ds(pl.multiple_of(d * keep, keep), keep)],
            tiles.at[i],
            load_sem.at[i],
        )

    fetch = pltpu.make_async_copy(coeffs, exact, exact_sem)
    fetch.start()
    for i in range(min(AHEAD, n * groups)):
        load(i).start()
    fetch.wait()

    whole = exact[...]
    high = whole.astype(jnp.bfloat16)
    rest = (whole - high.astype(jnp.float32)).astype(jnp.bfloat16)
    both = jnp.concatenate([high, rest], axis=0)
    tall, wide = spread.shape
    row = lax.broadcasted_iota(jnp.int32, (tall, 2 * widths), 0)
    col = lax.broadcasted_iota(jnp.int32, (tall, 2 * widths), 1)
    pick = jnp.where(row // GROUP == col, 1.0, 0.0).astype(jnp.bfloat16)
    row = lax.broadcasted_iota(jnp.int32, (count, wide), 0)
    col = lax.broadcasted_iota(jnp.int32, (count, wide), 1)
    repeat = jnp.where(col // GROUP == row, 1.0, 0.0).astype(jnp.bfloat16)
    tall_rows = jnp.dot(pick, both, preferred_element_type=jnp.float32).astype(jnp.bfloat16)
    full = jnp.dot(tall_rows, repeat, preferred_element_type=jnp.float32)
    row = lax.broadcasted_iota(jnp.int32, (GROUP, wide), 0)
    col = lax.broadcasted_iota(jnp.int32, (GROUP, wide), 1)
    same = (row == col % GROUP)[None]
    full = jnp.where(same, full.reshape(2 * widths, GROUP, wide), 0.0)
    spread[...] = full.reshape(tall, wide).astype(jnp.bfloat16)

    def copies(way, k, peer):
        code = pltpu.make_async_remote_copy(
            src_ref=out_code.at[way, k], dst_ref=in_code.at[way, k],
            send_sem=send_sem.at[way, k], recv_sem=recv_sem.at[way, k],
            device_id={"snap": peer}, device_id_type=MESH,
        )
        scale = pltpu.make_async_remote_copy(
            src_ref=out_scale.at[way, k], dst_ref=in_scale.at[way, k],
            send_sem=send_scale_sem.at[way, k], recv_sem=recv_scale_sem.at[way, k],
            device_id={"snap": peer}, device_id_type=MESH,
        )
        return scale, code

    def send(way, k, peer, value):
        code, scale = encode(value)
        out_code[way, k] = code
        out_scale[way, k] = scale
        for copy in copies(way, k, peer):
            copy.start()

    half = widths * GROUP

    @pl.loop(0, n * groups)
    def _(i):
        q, t = i // groups, lax.rem(i, groups)
        d = jnp.where(low, n - 1 - q, q)
        load(i).wait()

        @pl.when(i + AHEAD < n * groups)
        def _():
            load(i + AHEAD).start()

        both_parts = jnp.dot(
            spread[...], tiles[i].reshape(count * GROUP, keep), preferred_element_type=jnp.float32
        )
        value = (both_parts[:half] + both_parts[half:]).reshape(widths, GROUP, keep)
        part[d, t] = value

        @pl.when(i == 0)
        def _():
            pl.semaphore_wait(barrier, n - 1 + peers - 1)

        @pl.when(jnp.logical_and(jnp.logical_or(z == 0, z == n - 1), d != z))
        def _():
            way = jnp.where(z == 0, 0, 1)
            peer = jnp.where(z == 0, 1, n - 2)
            send(way, i, peer, value)

    @pl.loop(1, peers)
    def _(k):
        pl.semaphore_signal(known, inc=1, device_id={"param": lax.rem(me + k, peers)}, device_id_type=MESH)

    last = jnp.where(jnp.logical_or(jnp.logical_and(z > 0, 2 * z < n - 1), z == n - 1), 0, 1)

    def pass_on(way, k, d, peer):
        t = lax.rem(k, groups)
        for copy in copies(way, k, peer):
            copy.wait_recv()
        value = part[d, t] + decode(in_code[way, k], in_scale[way, k])

        @pl.when(d == z)
        def _():
            @pl.when(way != last)
            def _():
                part[d, t] = value

            @pl.when(way == last)
            def _():
                averages[:, pl.ds(pl.multiple_of(t * GROUP, GROUP), GROUP), :] = value
                squares[t] = jnp.sum(value * value, axis=1)

        @pl.when(d != z)
        def _():
            send(way, k, peer, value)

    @pl.loop(0, steps)
    def _(j):
        up = j - lag * (z - 1)

        @pl.when(jnp.logical_and(z > 0, jnp.logical_and(up >= 0, up < (n - z) * groups)))
        def _():
            pass_on(0, up, n - 1 - up // groups, jnp.where(z == n - 1, z - 1, z + 1))

        down = j - lag * (n - 2 - z)

        @pl.when(jnp.logical_and(z < n - 1, jnp.logical_and(down >= 0, down < (z + 1) * groups)))
        def _():
            pass_on(1, down, down // groups, jnp.where(z == 0, z + 1, z - 1))

    sums = jnp.sum(jnp.sum(squares[...], axis=0), axis=1, keepdims=True)
    lanes = norms.shape[1]
    row = lax.broadcasted_iota(jnp.int32, (widths, lanes), 0)
    col = lax.broadcasted_iota(jnp.int32, (widths, lanes), 1)
    line = jnp.sum(jnp.where(row == col, sums, 0.0), axis=0, keepdims=True)

    lines[z * peers + me] = line
    pl.semaphore_wait(known, peers - 1)

    def tell(j, k):
        place, peer = lax.rem(z + j, n), lax.rem(me + k, peers)
        return pltpu.make_async_remote_copy(
            src_ref=lines.at[z * peers + me], dst_ref=lines.at[z * peers + me],
            send_sem=line_send.at[j * peers + k], recv_sem=line_recv.at[z * peers + me],
            device_id={"snap": place, "param": peer}, device_id_type=MESH,
        )

    def hear(j, k):
        slot = lax.rem(z + j, n) * peers + lax.rem(me + k, peers)
        return pltpu.make_async_remote_copy(
            src_ref=lines.at[slot], dst_ref=lines.at[slot],
            send_sem=line_send.at[j * peers + k], recv_sem=line_recv.at[slot],
            device_id={"snap": lax.rem(z + j, n), "param": lax.rem(me + k, peers)}, device_id_type=MESH,
        )

    for j in range(n):
        @pl.loop(0 if j else 1, peers)
        def _(k):
            tell(j, k).start()

    for j in range(n):
        @pl.loop(0 if j else 1, peers)
        def _(k):
            hear(j, k).wait_recv()

    norms[...] = jnp.sqrt(jnp.sum(lines[...], axis=0) / jnp.float32(entries))

    for j in range(n):
        @pl.loop(0 if j else 1, peers)
        def _(k):
            tell(j, k).wait_send()

    @pl.loop(0, steps)
    def _(k):
        @pl.when(k < (n - 1 - z) * groups)
        def _():
            for copy in copies(0, k, jnp.where(z == n - 1, z - 1, z + 1)):
                copy.wait_send()

        @pl.when(k < z * groups)
        def _():
            for copy in copies(1, k, jnp.where(z == 0, z + 1, z - 1)):
                copy.wait_send()


def on_device(n, peers, snapshots, coeffs):
    count, height, cols = snapshots.shape
    widths = coeffs.shape[0]
    keep = cols // n
    groups = height // GROUP
    steps = (n - 1) * groups
    entries = height * cols * peers
    dma = pltpu.SemaphoreType.DMA
    averages, norms = pl.pallas_call(
        functools.partial(kernel, n, peers, entries),
        out_shape=(
            jax.ShapeDtypeStruct((widths, height, keep), jnp.float32),
            jax.ShapeDtypeStruct((1, 128), jnp.float32),
        ),
        in_specs=[pl.BlockSpec(memory_space=pltpu.HBM)] * 2,
        out_specs=(pl.BlockSpec(memory_space=pltpu.VMEM), pl.BlockSpec(memory_space=pltpu.VMEM)),
        scratch_shapes=[
            pltpu.VMEM((widths, count), jnp.float32),
            pltpu.VMEM((2 * widths * GROUP, count * GROUP), jnp.bfloat16),
            pltpu.VMEM((n * groups, count, GROUP, keep), jnp.bfloat16),
            pltpu.VMEM((n, groups, widths, GROUP, keep), jnp.float32),
            pltpu.VMEM((2, steps, widths, GROUP, keep), jnp.bfloat16),
            pltpu.VMEM((2, steps, 1, keep), jnp.float32),
            pltpu.VMEM((2, steps, widths, GROUP, keep), jnp.bfloat16),
            pltpu.VMEM((2, steps, 1, keep), jnp.float32),
            pltpu.VMEM((groups, widths, keep), jnp.float32),
            pltpu.VMEM((n * peers, 1, 128), jnp.float32),
            dma(()),
            dma((n * groups,)),
            dma((2, steps)), dma((2, steps)), dma((2, steps)), dma((2, steps)),
            dma((n * peers,)), dma((n * peers,)), pltpu.SemaphoreType.REGULAR,
        ],
        compiler_params=pltpu.CompilerParams(
            collective_id=0, has_side_effects=True, vmem_limit_bytes=48 * 1024 * 1024
        ),
        name="reconstruct",
    )(coeffs, snapshots)
    return averages, norms[0, :widths]


def solution(mesh):
    in_specs = (P("snap", "param", None), P(None, "snap"))
    out_specs = (P(None, "param", "snap"), P())
    body = functools.partial(on_device, mesh.shape["snap"], mesh.shape["param"])
    return jax.shard_map(body, mesh=mesh, in_specs=in_specs, out_specs=out_specs, check_vma=False)
```

```python
import functools

import jax
import jax.numpy as jnp
from jax import lax
from jax.experimental import pallas as pl
from jax.experimental.pallas import tpu as pltpu
from jax.sharding import PartitionSpec as P

MESH = pl.DeviceIdType.MESH
GROUP = 16
LAG = 3
POWER = 15
AHEAD = 4
TOP = 2.0**8.375


def encode(value):
    largest = jnp.max(jnp.max(jnp.abs(value), axis=0), axis=0, keepdims=True)
    largest = jnp.maximum(largest, 1e-30)
    x = value * (TOP / largest)[None]
    x2 = x * x
    x4 = x2 * x2
    x8 = x4 * x4
    return ((x8 * x4) * (x2 * x)).astype(jnp.bfloat16), largest * (1.0 / TOP)


def decode(code, scale):
    y = code.astype(jnp.float32)
    size = jnp.exp2(jnp.log2(jnp.maximum(jnp.abs(y), 1e-38)) * (1.0 / POWER)) * scale[None]
    return jnp.where(y > 0.0, size, jnp.where(y < 0.0, -size, 0.0))


def each(size, body):
    if size <= 8:
        for k in range(size):
            body(k)
    else:
        pl.loop(0, size)(body)


def kernel(
    n, peers, entries, coeffs, stored, averages, norms,
    spread, tiles, part, out_code, out_scale, in_code, in_scale, squares, lines,
    load_sem, send_sem, send_scale_sem, recv_sem, recv_scale_sem,
    line_send, line_recv, known,
):
    z = lax.axis_index("snap")
    me = lax.axis_index("param")
    widths, count = coeffs.shape
    keep = stored.shape[2] // n
    groups = stored.shape[1] // GROUP
    steps = (n - 1) * groups
    lag = min(LAG, groups - 1)
    low = z < n // 2

    def load(i):
        q, t = i // groups, lax.rem(i, groups)
        d = jnp.where(low, n - 1 - q, q)
        return pltpu.make_async_copy(
            stored.at[:, pl.ds(pl.multiple_of(t * GROUP, GROUP), GROUP), pl.ds(pl.multiple_of(d * keep, keep), keep)],
            tiles.at[i],
            load_sem.at[i],
        )

    load(0).start()
    barrier = pltpu.get_barrier_semaphore()

    def greet(axis, mine):
        def body(k):
            @pl.when(k != mine)
            def _():
                pl.semaphore_signal(barrier, inc=1, device_id={axis: k}, device_id_type=MESH)

        return body

    each(n, greet("snap", z))
    each(peers, greet("param", me))
    for i in range(1, min(AHEAD, n * groups)):
        load(i).start()

    whole = coeffs[...]
    high = whole.astype(jnp.bfloat16)
    rest = (whole - high.astype(jnp.float32)).astype(jnp.bfloat16)
    both = jnp.concatenate([high, rest], axis=0)
    tall, wide = spread.shape
    row = lax.broadcasted_iota(jnp.int32, (tall, 2 * widths), 0)
    col = lax.broadcasted_iota(jnp.int32, (tall, 2 * widths), 1)
    pick = jnp.where(row // GROUP == col, 1.0, 0.0).astype(jnp.bfloat16)
    row = lax.broadcasted_iota(jnp.int32, (count, wide), 0)
    col = lax.broadcasted_iota(jnp.int32, (count, wide), 1)
    repeat = jnp.where(col // GROUP == row, 1.0, 0.0).astype(jnp.bfloat16)
    tall_rows = jnp.dot(pick, both, preferred_element_type=jnp.float32).astype(jnp.bfloat16)
    full = jnp.dot(tall_rows, repeat, preferred_element_type=jnp.float32)
    row = lax.broadcasted_iota(jnp.int32, (GROUP, wide), 0)
    col = lax.broadcasted_iota(jnp.int32, (GROUP, wide), 1)
    same = (row == col % GROUP)[None]
    full = jnp.where(same, full.reshape(2 * widths, GROUP, wide), 0.0)
    spread[...] = full.reshape(tall, wide).astype(jnp.bfloat16)

    def copies(way, k, peer):
        code = pltpu.make_async_remote_copy(
            src_ref=out_code.at[way, k], dst_ref=in_code.at[way, k],
            send_sem=send_sem.at[way, k], recv_sem=recv_sem.at[way, k],
            device_id={"snap": peer}, device_id_type=MESH,
        )
        scale = pltpu.make_async_remote_copy(
            src_ref=out_scale.at[way, k], dst_ref=in_scale.at[way, k],
            send_sem=send_scale_sem.at[way, k], recv_sem=recv_scale_sem.at[way, k],
            device_id={"snap": peer}, device_id_type=MESH,
        )
        return scale, code

    def send(way, k, peer, value):
        code, scale = encode(value)
        out_code[way, k] = code
        out_scale[way, k] = scale
        for copy in copies(way, k, peer):
            copy.start()

    half = widths * GROUP

    @pl.loop(0, n * groups)
    def _(i):
        q, t = i // groups, lax.rem(i, groups)
        d = jnp.where(low, n - 1 - q, q)
        load(i).wait()

        @pl.when(i + AHEAD < n * groups)
        def _():
            load(i + AHEAD).start()

        both_parts = jnp.dot(
            spread[...], tiles[i].reshape(count * GROUP, keep), preferred_element_type=jnp.float32
        )
        value = (both_parts[:half] + both_parts[half:]).reshape(widths, GROUP, keep)
        part[d, t] = value

        @pl.when(i == 0)
        def _():
            pl.semaphore_wait(barrier, n - 1 + peers - 1)

        @pl.when(jnp.logical_and(jnp.logical_or(z == 0, z == n - 1), d != z))
        def _():
            way = jnp.where(z == 0, 0, 1)
            peer = jnp.where(z == 0, 1, n - 2)
            send(way, i, peer, value)

    def inform(k):
        @pl.when(k != me)
        def _():
            pl.semaphore_signal(known, inc=1, device_id={"param": k}, device_id_type=MESH)

    each(peers, inform)

    last = jnp.where(jnp.logical_or(jnp.logical_and(z > 0, 2 * z < n - 1), z == n - 1), 0, 1)

    def pass_on(way, k, d, peer):
        t = lax.rem(k, groups)
        for copy in copies(way, k, peer):
            copy.wait_recv()
        value = part[d, t] + decode(in_code[way, k], in_scale[way, k])

        @pl.when(d == z)
        def _():
            @pl.when(way != last)
            def _():
                part[d, t] = value

            @pl.when(way == last)
            def _():
                averages[:, pl.ds(pl.multiple_of(t * GROUP, GROUP), GROUP), :] = value
                squares[t] = jnp.sum(value * value, axis=1)

        @pl.when(d != z)
        def _():
            send(way, k, peer, value)

    @pl.loop(0, steps)
    def _(j):
        up = j - lag * (z - 1)

        @pl.when(jnp.logical_and(z > 0, jnp.logical_and(up >= 0, up < (n - z) * groups)))
        def _():
            pass_on(0, up, n - 1 - up // groups, jnp.where(z == n - 1, z - 1, z + 1))

        down = j - lag * (n - 2 - z)

        @pl.when(jnp.logical_and(z < n - 1, jnp.logical_and(down >= 0, down < (z + 1) * groups)))
        def _():
            pass_on(1, down, down // groups, jnp.where(z == 0, z + 1, z - 1))

    sums = jnp.sum(jnp.sum(squares[...], axis=0), axis=1, keepdims=True)
    lanes = norms.shape[1]
    row = lax.broadcasted_iota(jnp.int32, (widths, lanes), 0)
    col = lax.broadcasted_iota(jnp.int32, (widths, lanes), 1)
    line = jnp.sum(jnp.where(row == col, sums, 0.0), axis=0, keepdims=True)

    own = z * peers + me
    lines[own] = line
    pl.semaphore_wait(known, peers - 1)

    def others(act):
        for p in range(n):
            def body(k, p=p):
                @pl.when(jnp.logical_or(p != z, k != me))
                def _():
                    act(p, k)

            each(peers, body)

    def line_copy(p, k, slot):
        return pltpu.make_async_remote_copy(
            src_ref=lines.at[slot], dst_ref=lines.at[slot],
            send_sem=line_send.at[p * peers + k], recv_sem=line_recv.at[slot],
            device_id={"snap": p, "param": k}, device_id_type=MESH,
        )

    others(lambda p, k: line_copy(p, k, own).start())

    @pl.loop(0, steps)
    def _(k):
        @pl.when(k < (n - 1 - z) * groups)
        def _():
            for copy in copies(0, k, jnp.where(z == n - 1, z - 1, z + 1)):
                copy.wait_send()

        @pl.when(k < z * groups)
        def _():
            for copy in copies(1, k, jnp.where(z == 0, z + 1, z - 1)):
                copy.wait_send()

    others(lambda p, k: line_copy(p, k, own).wait_send())
    others(lambda p, k: line_copy(p, k, p * peers + k).wait_recv())
    norms[...] = jnp.sqrt(jnp.sum(lines[...], axis=0) / jnp.float32(entries))


def on_device(n, peers, snapshots, coeffs):
    count, height, cols = snapshots.shape
    widths = coeffs.shape[0]
    keep = cols // n
    groups = height // GROUP
    steps = (n - 1) * groups
    entries = height * cols * peers
    dma = pltpu.SemaphoreType.DMA
    averages, norms = pl.pallas_call(
        functools.partial(kernel, n, peers, entries),
        out_shape=(
            jax.ShapeDtypeStruct((widths, height, keep), jnp.float32),
            jax.ShapeDtypeStruct((1, 128), jnp.float32),
        ),
        in_specs=[pl.BlockSpec(memory_space=pltpu.VMEM), pl.BlockSpec(memory_space=pl.ANY)],
        out_specs=(pl.BlockSpec(memory_space=pltpu.VMEM), pl.BlockSpec(memory_space=pltpu.VMEM)),
        scratch_shapes=[
            pltpu.VMEM((2 * widths * GROUP, count * GROUP), jnp.bfloat16),
            pltpu.VMEM((n * groups, count, GROUP, keep), jnp.bfloat16),
            pltpu.VMEM((n, groups, widths, GROUP, keep), jnp.float32),
            pltpu.VMEM((2, steps, widths, GROUP, keep), jnp.bfloat16),
            pltpu.VMEM((2, steps, 1, keep), jnp.float32),
            pltpu.VMEM((2, steps, widths, GROUP, keep), jnp.bfloat16),
            pltpu.VMEM((2, steps, 1, keep), jnp.float32),
            pltpu.VMEM((groups, widths, keep), jnp.float32),
            pltpu.VMEM((n * peers, 1, 128), jnp.float32),
            dma((n * groups,)),
            dma((2, steps)), dma((2, steps)), dma((2, steps)), dma((2, steps)),
            dma((n * peers,)), dma((n * peers,)), pltpu.SemaphoreType.REGULAR,
        ],
        compiler_params=pltpu.CompilerParams(
            collective_id=0, has_side_effects=True, vmem_limit_bytes=48 * 1024 * 1024
        ),
        name="reconstruct",
    )(coeffs, snapshots)
    return averages, norms[0, :widths]


def solution(mesh):
    in_specs = (P("snap", "param", None), P(None, "snap"))
    out_specs = (P(None, "param", "snap"), P())
    body = functools.partial(on_device, mesh.shape["snap"], mesh.shape["param"])
    return jax.shard_map(body, mesh=mesh, in_specs=in_specs, out_specs=out_specs, check_vma=False)
```

```python
import functools

import jax
import jax.numpy as jnp
from jax import lax
from jax.experimental import pallas as pl
from jax.experimental.pallas import tpu as pltpu
from jax.sharding import PartitionSpec as P

MESH = pl.DeviceIdType.MESH
GROUP = 16
LAG = 3
POWER = 15
AHEAD = 4
TOP = 2.0**8.375


def encode(value):
    largest = jnp.max(jnp.max(jnp.abs(value), axis=0), axis=0, keepdims=True)
    largest = jnp.maximum(largest, 1e-30)
    x = value * (TOP / largest)[None]
    x2 = x * x
    x4 = x2 * x2
    x8 = x4 * x4
    return ((x8 * x4) * (x2 * x)).astype(jnp.bfloat16), largest * (1.0 / TOP)


def decode(code, scale):
    y = code.astype(jnp.float32)
    size = jnp.exp2(jnp.log2(jnp.maximum(jnp.abs(y), 1e-38)) * (1.0 / POWER)) * scale[None]
    return jnp.where(y > 0.0, size, jnp.where(y < 0.0, -size, 0.0))


def each(size, body):
    if size <= 8:
        for k in range(size):
            body(k)
    else:
        pl.loop(0, size)(body)


def serves(p, n):
    return jnp.logical_and(p + 1 <= n - 2, 2 * (p + 1) < n - 1), jnp.logical_and(p - 1 >= 1, 2 * (p - 1) >= n - 1)


def has_line(p, n):
    return p in (0, n - 1) or 2 * (p + 1) < n - 1 or 2 * (p - 1) >= n - 1


def kernel(
    n, peers, entries, coeffs, stored, averages, norms,
    spread, tiles, part, out_code, out_scale, in_code, in_scale,
    back_out, back_out_scale, back_in, back_in_scale, squares, lines,
    load_sem, send_sem, send_scale_sem, recv_sem, recv_scale_sem,
    back_sem, back_scale_sem, back_recv, back_recv_scale, line_send, line_recv, known,
):
    z = lax.axis_index("snap")
    me = lax.axis_index("param")
    widths, count = coeffs.shape
    keep = stored.shape[2] // n
    groups = stored.shape[1] // GROUP
    steps = (n - 1) * groups
    lag = min(LAG, groups - 1)
    low = z < n // 2

    def load(i):
        q, t = i // groups, lax.rem(i, groups)
        d = jnp.where(low, n - 1 - q, q)
        return pltpu.make_async_copy(
            stored.at[:, pl.ds(pl.multiple_of(t * GROUP, GROUP), GROUP), pl.ds(pl.multiple_of(d * keep, keep), keep)],
            tiles.at[i],
            load_sem.at[i],
        )

    load(0).start()
    squares[...] = jnp.zeros_like(squares)
    barrier = pltpu.get_barrier_semaphore()

    def greet(axis, mine):
        def body(k):
            @pl.when(k != mine)
            def _():
                pl.semaphore_signal(barrier, inc=1, device_id={axis: k}, device_id_type=MESH)

        return body

    each(n, greet("snap", z))
    each(peers, greet("param", me))
    for i in range(1, min(AHEAD, n * groups)):
        load(i).start()

    whole = coeffs[...]
    high = whole.astype(jnp.bfloat16)
    rest = (whole - high.astype(jnp.float32)).astype(jnp.bfloat16)
    both = jnp.concatenate([high, rest], axis=0)
    tall, wide = spread.shape
    row = lax.broadcasted_iota(jnp.int32, (tall, 2 * widths), 0)
    col = lax.broadcasted_iota(jnp.int32, (tall, 2 * widths), 1)
    pick = jnp.where(row // GROUP == col, 1.0, 0.0).astype(jnp.bfloat16)
    row = lax.broadcasted_iota(jnp.int32, (count, wide), 0)
    col = lax.broadcasted_iota(jnp.int32, (count, wide), 1)
    repeat = jnp.where(col // GROUP == row, 1.0, 0.0).astype(jnp.bfloat16)
    tall_rows = jnp.dot(pick, both, preferred_element_type=jnp.float32).astype(jnp.bfloat16)
    full = jnp.dot(tall_rows, repeat, preferred_element_type=jnp.float32)
    row = lax.broadcasted_iota(jnp.int32, (GROUP, wide), 0)
    col = lax.broadcasted_iota(jnp.int32, (GROUP, wide), 1)
    same = (row == col % GROUP)[None]
    full = jnp.where(same, full.reshape(2 * widths, GROUP, wide), 0.0)
    spread[...] = full.reshape(tall, wide).astype(jnp.bfloat16)

    def copies(way, k, peer):
        code = pltpu.make_async_remote_copy(
            src_ref=out_code.at[way, k], dst_ref=in_code.at[way, k],
            send_sem=send_sem.at[way, k], recv_sem=recv_sem.at[way, k],
            device_id={"snap": peer}, device_id_type=MESH,
        )
        scale = pltpu.make_async_remote_copy(
            src_ref=out_scale.at[way, k], dst_ref=in_scale.at[way, k],
            send_sem=send_scale_sem.at[way, k], recv_sem=recv_scale_sem.at[way, k],
            device_id={"snap": peer}, device_id_type=MESH,
        )
        return scale, code

    def send(way, k, peer, value):
        code, scale = encode(value)
        out_code[way, k] = code
        out_scale[way, k] = scale
        for copy in copies(way, k, peer):
            copy.start()

    half = widths * GROUP

    @pl.loop(0, n * groups)
    def _(i):
        q, t = i // groups, lax.rem(i, groups)
        d = jnp.where(low, n - 1 - q, q)
        load(i).wait()

        @pl.when(i + AHEAD < n * groups)
        def _():
            load(i + AHEAD).start()

        both_parts = jnp.dot(
            spread[...], tiles[i].reshape(count * GROUP, keep), preferred_element_type=jnp.float32
        )
        value = (both_parts[:half] + both_parts[half:]).reshape(widths, GROUP, keep)
        part[d, t] = value

        @pl.when(i == 0)
        def _():
            pl.semaphore_wait(barrier, n - 1 + peers - 1)

        @pl.when(jnp.logical_and(jnp.logical_or(z == 0, z == n - 1), d != z))
        def _():
            way = jnp.where(z == 0, 0, 1)
            peer = jnp.where(z == 0, 1, n - 2)
            send(way, i, peer, value)

    def inform(k):
        @pl.when(k != me)
        def _():
            pl.semaphore_signal(known, inc=1, device_id={"param": k}, device_id_type=MESH)

    each(peers, inform)

    last = jnp.where(jnp.logical_or(jnp.logical_and(z > 0, 2 * z < n - 1), z == n - 1), 0, 1)

    inner = jnp.logical_and(z > 0, z < n - 1)
    above, below = serves(z, n)

    def back_copies(t, peer):
        code = pltpu.make_async_remote_copy(
            src_ref=back_out.at[t], dst_ref=back_in.at[t],
            send_sem=back_sem.at[t], recv_sem=back_recv.at[t],
            device_id={"snap": peer}, device_id_type=MESH,
        )
        scale = pltpu.make_async_remote_copy(
            src_ref=back_out_scale.at[t], dst_ref=back_in_scale.at[t],
            send_sem=back_scale_sem.at[t], recv_sem=back_recv_scale.at[t],
            device_id={"snap": peer}, device_id_type=MESH,
        )
        return scale, code

    outward = jnp.where(jnp.logical_and(inner, last == 0), z - 1, jnp.where(inner, z + 1, jnp.where(z == 0, 1, n - 2)))

    def pass_on(way, k, d, peer):
        t = lax.rem(k, groups)
        for copy in copies(way, k, peer):
            copy.wait_recv()
        value = part[d, t] + decode(in_code[way, k], in_scale[way, k])

        @pl.when(d == z)
        def _():
            @pl.when(way != last)
            def _():
                part[d, t] = value
                code, scale = encode(value)
                back_out[t] = code
                back_out_scale[t] = scale
                for copy in back_copies(t, outward):
                    copy.start()

            @pl.when(way == last)
            def _():
                averages[:, pl.ds(pl.multiple_of(t * GROUP, GROUP), GROUP), :] = value

                @pl.when(jnp.logical_not(inner))
                def _():
                    squares[t] = jnp.sum(value * value, axis=1)

        @pl.when(d != z)
        def _():
            part[d, t] = value
            send(way, k, peer, value)

    @pl.loop(0, steps)
    def _(j):
        up = j - lag * (z - 1)

        @pl.when(jnp.logical_and(z > 0, jnp.logical_and(up >= 0, up < (n - z) * groups)))
        def _():
            pass_on(0, up, n - 1 - up // groups, jnp.where(z == n - 1, z - 1, z + 1))

        down = j - lag * (n - 2 - z)

        @pl.when(jnp.logical_and(z < n - 1, jnp.logical_and(down >= 0, down < (z + 1) * groups)))
        def _():
            pass_on(1, down, down // groups, jnp.where(z == 0, z + 1, z - 1))

    @pl.when(jnp.logical_or(above, below))
    def _():
        served = jnp.where(above, z + 1, z - 1)

        @pl.loop(0, groups)
        def _(t):
            for copy in back_copies(t, served):
                copy.wait_recv()
            value = part[served, t] + decode(back_in[t], back_in_scale[t])
            squares[groups + t] = jnp.sum(value * value, axis=1)

    sums = jnp.sum(jnp.sum(squares[...], axis=0), axis=1, keepdims=True)
    lanes = norms.shape[1]
    row = lax.broadcasted_iota(jnp.int32, (widths, lanes), 0)
    col = lax.broadcasted_iota(jnp.int32, (widths, lanes), 1)
    line = jnp.sum(jnp.where(row == col, sums, 0.0), axis=0, keepdims=True)

    own = z * peers + me
    lines[own] = line
    pl.semaphore_wait(known, peers - 1)

    def others(act, places):
        for p in places:
            def body(k, p=p):
                @pl.when(jnp.logical_or(p != z, k != me))
                def _():
                    act(p, k)

            each(peers, body)

    tellers = [p for p in range(n) if has_line(p, n)]
    tells = functools.reduce(jnp.logical_or, [z == p for p in tellers])

    def line_copy(p, k, slot):
        return pltpu.make_async_remote_copy(
            src_ref=lines.at[slot], dst_ref=lines.at[slot],
            send_sem=line_send.at[p * peers + k], recv_sem=line_recv.at[slot],
            device_id={"snap": p, "param": k}, device_id_type=MESH,
        )

    @pl.when(tells)
    def _():
        others(lambda p, k: line_copy(p, k, own).start(), range(n))


    @pl.loop(0, steps)
    def _(k):
        @pl.when(k < (n - 1 - z) * groups)
        def _():
            for copy in copies(0, k, jnp.where(z == n - 1, z - 1, z + 1)):
                copy.wait_send()

        @pl.when(k < z * groups)
        def _():
            for copy in copies(1, k, jnp.where(z == 0, z + 1, z - 1)):
                copy.wait_send()

    @pl.when(inner)
    def _():
        @pl.loop(0, groups)
        def _(t):
            for copy in back_copies(t, outward):
                copy.wait_send()

    @pl.when(tells)
    def _():
        others(lambda p, k: line_copy(p, k, own).wait_send(), range(n))

    others(lambda p, k: line_copy(p, k, p * peers + k).wait_recv(), tellers)
    total = jnp.zeros_like(line)
    for p in tellers:
        total += jnp.sum(lines[p * peers : (p + 1) * peers], axis=0)
    norms[...] = jnp.sqrt(total / jnp.float32(entries))


def on_device(n, peers, snapshots, coeffs):
    count, height, cols = snapshots.shape
    widths = coeffs.shape[0]
    keep = cols // n
    groups = height // GROUP
    steps = (n - 1) * groups
    entries = height * cols * peers
    dma = pltpu.SemaphoreType.DMA
    averages, norms = pl.pallas_call(
        functools.partial(kernel, n, peers, entries),
        out_shape=(
            jax.ShapeDtypeStruct((widths, height, keep), jnp.float32),
            jax.ShapeDtypeStruct((1, 128), jnp.float32),
        ),
        in_specs=[pl.BlockSpec(memory_space=pltpu.VMEM), pl.BlockSpec(memory_space=pl.ANY)],
        out_specs=(pl.BlockSpec(memory_space=pltpu.VMEM), pl.BlockSpec(memory_space=pltpu.VMEM)),
        scratch_shapes=[
            pltpu.VMEM((2 * widths * GROUP, count * GROUP), jnp.bfloat16),
            pltpu.VMEM((n * groups, count, GROUP, keep), jnp.bfloat16),
            pltpu.VMEM((n, groups, widths, GROUP, keep), jnp.float32),
            pltpu.VMEM((2, steps, widths, GROUP, keep), jnp.bfloat16),
            pltpu.VMEM((2, steps, 1, keep), jnp.float32),
            pltpu.VMEM((2, steps, widths, GROUP, keep), jnp.bfloat16),
            pltpu.VMEM((2, steps, 1, keep), jnp.float32),
            pltpu.VMEM((groups, widths, GROUP, keep), jnp.bfloat16),
            pltpu.VMEM((groups, 1, keep), jnp.float32),
            pltpu.VMEM((groups, widths, GROUP, keep), jnp.bfloat16),
            pltpu.VMEM((groups, 1, keep), jnp.float32),
            pltpu.VMEM((2 * groups, widths, keep), jnp.float32),
            pltpu.VMEM((n * peers, 1, 128), jnp.float32),
            dma((n * groups,)),
            dma((2, steps)), dma((2, steps)), dma((2, steps)), dma((2, steps)),
            dma((groups,)), dma((groups,)), dma((groups,)), dma((groups,)),
            dma((n * peers,)), dma((n * peers,)), pltpu.SemaphoreType.REGULAR,
        ],
        compiler_params=pltpu.CompilerParams(
            collective_id=0, has_side_effects=True, vmem_limit_bytes=48 * 1024 * 1024
        ),
        name="reconstruct",
    )(coeffs, snapshots)
    return averages, norms[0, :widths]


def solution(mesh):
    in_specs = (P("snap", "param", None), P(None, "snap"))
    out_specs = (P(None, "param", "snap"), P())
    body = functools.partial(on_device, mesh.shape["snap"], mesh.shape["param"])
    return jax.shard_map(body, mesh=mesh, in_specs=in_specs, out_specs=out_specs, check_vma=False)
```
